32 devices in a mesh: dp: 4 (over z), ctx: 8 (over y, x, core).
Axes of the slice: x: 2, y: 2, z: 4, core: 2. Of those that a mesh axis runs over, the one named last changes fastest.
Arguments:
- item_ids: int32 [16, 2048], P('dp', 'ctx'), may hold values from 0 to 65535, as said below
- lengths: int32 [16], P('dp'), may hold values from 256 to 2048
- table: bfloat16 [65536, 512], P('dp'), may hold values from -6 to 6
- w_in: bfloat16 [512, 2048], replicated, may hold values from -0.25 to 0.25
- w_out: bfloat16 [512, 512], replicated, may hold values from -0.25 to 0.25
Outputs:
- layer_out: bfloat16 [16, 2048, 512], P('dp', 'ctx')
The draws below stay inside these ranges and needn't reach their ends.
Inputs may be any that keep to these rules, and one draw needn't show every extreme that they name: `item_ids`: the owner of an id is id // 16384. In every user's block of 256 positions of one index of ctx, at most 128 ids have one owner; in each such block one owner, the same for all users at that index of ctx, has exactly 128.
All inputs are finite; a program needn't handle non-finite values.
Results may differ from the reference program's by a relative error of at most 0.0054.
Values may be sent and summed in bfloat16 or wider, within the bound.
A program may use at most 128 MiB of HBM per device.

```python
import math
import jax
import jax.numpy as jnp
from jax import lax

D = 512
HEADS = 8
BLK = 256
VOC_DEV = 16384
SEQ = 2048
USERS = 16
VOCAB = 65536
CAP = 128


def draw_item_ids(key, part):
    owner_count = VOCAB // VOC_DEV
    block_count = SEQ // BLK
    hottest = jax.random.randint(jax.random.fold_in(key, 1), (block_count,), 0, owner_count).astype(jnp.int32)

    def one_block(user, block, hot_owner):
        block_key = jax.random.fold_in(jax.random.fold_in(key, 2), user * block_count + block)
        key_slots = jax.random.fold_in(block_key, 3)
        key_order = jax.random.fold_in(block_key, 4)
        key_top = jax.random.fold_in(block_key, 5)
        key_rows = jax.random.fold_in(block_key, 6)
        slots = jax.random.permutation(key_slots, (owner_count - 1) * CAP)[:BLK - CAP].astype(jnp.int32)
        others = slots // CAP
        others = others + (others >= hot_owner).astype(jnp.int32)
        owners = jnp.concatenate([jnp.full((CAP,), hot_owner, jnp.int32), others])
        owners = jax.random.permutation(key_order, owners)
        upper = jax.random.randint(key_top, (BLK,), 1, VOC_DEV + 1)
        rows = jax.random.randint(key_rows, (BLK,), 0, upper)
        return (owners * VOC_DEV + rows).astype(jnp.int32)
    users = jnp.arange(USERS, dtype=jnp.int32)
    blocks = jnp.arange(block_count, dtype=jnp.int32)
    per_user = jax.vmap(lambda user: jax.vmap(lambda block, hot_owner: one_block(user, block, hot_owner))(blocks, hottest))
    drawn = per_user(users)
    return drawn.reshape(USERS, SEQ)


def set_ends(result, key, smallest, top_value):
    shape = result.shape
    index_at = [jax.random.randint(jax.random.fold_in(key, axis), (), 0, shape[axis]) for axis in range(len(shape))]
    result = result.at[tuple(index_at)].set(smallest)
    longest = shape.index(max(shape))
    index_at[longest] = (index_at[longest] + 1) % shape[longest]
    return result.at[tuple(index_at)].set(top_value)


def steps_of(stream_key, extent, pieces, low, largest):
    def one(axis_at, shards_of):
        heights = jax.random.uniform(jax.random.fold_in(jax.random.fold_in(stream_key, 6), axis_at), (shards_of,), jnp.float32, low / len(pieces), largest / len(pieces))
        return jnp.repeat(jnp.exp(heights), extent[axis_at] // shards_of).reshape((-1,) + (1,) * (len(extent) - axis_at - 1))

    factor_of = one(*pieces[0])
    for cut in pieces[1:]:
        factor_of = factor_of * one(*cut)
    return factor_of


def normal_values(own_key, dims, width, reach, pieces=(), kind=jnp.bfloat16):
    values = jax.random.normal(own_key, dims, jnp.float32) * width
    if len(pieces) > 0:
        values = steps_of(own_key, dims, pieces, -0.22, 0.18) * values
    return jnp.clip(values, min=-reach, max=reach).astype(kind)


def setup_inputs(seed: int = 0) -> dict:
    key_of = jax.random.split(jax.random.key(seed), 6)
    return {
        "item_ids": draw_item_ids(jax.random.fold_in(key_of[5], 71), 0),
        "lengths": set_ends(jax.random.randint(key_of[1], (USERS,), SEQ // 8, SEQ + 1), jax.random.fold_in(key_of[1], 1), SEQ // 8, SEQ).astype(jnp.int32),
        "table": normal_values(key_of[2], (VOCAB, D), 1.0, 6.0, ((0, 4),)),
        "w_in": normal_values(key_of[3], (D, 4 * D), D ** -0.5, 0.25),
        "w_out": normal_values(key_of[4], (D, D), D ** -0.5, 0.25),
    }


def layer_norm(values):
    center = values - lax.optimization_barrier(jnp.mean(values, axis=-1, keepdims=True))
    spread = lax.optimization_barrier(jnp.mean(center * center, axis=-1, keepdims=True))
    return center * lax.rsqrt(spread + 1e-05)

def reference(item_ids, lengths, table, w_in, w_out):
    embedded = jnp.take(table, item_ids, axis=0)
    normed = layer_norm(embedded.astype(jnp.float32)).astype(jnp.bfloat16)
    projected = jax.nn.silu(jnp.dot(normed.reshape(-1, D), w_in, preferred_element_type=jnp.float32))
    projected = projected.astype(jnp.bfloat16).reshape(USERS, SEQ, 4 * D)
    gate_rows = projected[..., :D]
    value_rows = projected[..., D:2 * D]
    query_rows = projected[..., 2 * D:3 * D]
    key_rows = projected[..., 3 * D:]
    head_size = D // HEADS
    query_block = math.gcd(SEQ, 512)

    def one_user(packed):
        user_queries, user_keys, user_values, length_one = packed
        outputs = []
        for block_index in range(SEQ // query_block):
            row_low = block_index * query_block
            row_high = row_low + query_block
            query_heads = user_queries[row_low:row_high].astype(jnp.float32).reshape(query_block, HEADS, head_size)
            key_heads = user_keys[:row_high].astype(jnp.float32).reshape(row_high, HEADS, head_size)
            value_heads = user_values[:row_high].astype(jnp.float32).reshape(row_high, HEADS, head_size)
            scores = jnp.einsum('qhd,khd->hqk', query_heads, key_heads) * (1.0 / math.sqrt(head_size))
            query_pos = row_low + jnp.arange(query_block, dtype=jnp.int32)
            key_pos = jnp.arange(row_high, dtype=jnp.int32)
            visible = (key_pos[None, :] <= query_pos[:, None]) & (key_pos[None, :] < length_one)
            weights = jnp.where(visible[None], jax.nn.silu(scores), 0.0).astype(jnp.bfloat16)
            attended = jnp.einsum('hqk,khd->qhd', weights.astype(jnp.float32), value_heads)
            outputs.append(attended.reshape(query_block, D))
        return jnp.concatenate(outputs, axis=0)
    attended = lax.map(one_user, (query_rows, key_rows, value_rows, lengths))
    gated = (layer_norm(attended) * gate_rows.astype(jnp.float32)).astype(jnp.bfloat16)
    mixed = jnp.dot(gated.reshape(-1, D), w_out, preferred_element_type=jnp.float32).reshape(USERS, SEQ, D)
    return (embedded.astype(jnp.float32) + mixed).astype(jnp.bfloat16)
```

```python
import functools
import math

import jax
import jax.numpy as jnp
from jax import lax
from jax.experimental import pallas as pl
from jax.experimental.pallas import tpu as pltpu
from jax.sharding import PartitionSpec as P

HEADS = 8
F32 = jnp.float32
BF16 = jnp.bfloat16
MESH = pl.DeviceIdType.MESH


def half_silu(h):
    return h + h * jnp.tanh(h)


def greet(axis, size, me, other):
    barrier = pltpu.get_barrier_semaphore()
    for step in range(1, size):
        peer = lax.rem(me + step, size)
        device = (peer, other) if axis == "dp" else (other, peer)
        pl.semaphore_signal(barrier, inc=1, device_id=device, device_id_type=MESH)


def index_kernel(owners, owned, cap, ids_ref, index_ref, slot_ref, ids_all, send_sem, recv_sem):
    users, _, rows = ids_ref.shape
    my_dp, my_ctx = lax.axis_index("dp"), lax.axis_index("ctx")
    greet("dp", owners, my_dp, my_ctx)
    pl.semaphore_wait(pltpu.get_barrier_semaphore(), owners - 1)
    copies = []
    for step in range(1, owners):
        copies.append(
            pltpu.make_async_remote_copy(
                src_ref=ids_ref,
                dst_ref=ids_all.at[my_dp],
                send_sem=send_sem.at[step],
                recv_sem=recv_sem.at[step],
                device_id=(lax.rem(my_dp + step, owners), my_ctx),
                device_id_type=MESH,
            )
        )
        copies[-1].start()
    earlier = lax.broadcasted_iota(jnp.int32, (rows, rows), 0)
    later = lax.broadcasted_iota(jnp.int32, (rows, rows), 1)
    upto = (earlier <= later).astype(BF16)
    own = ids_ref[...].reshape(users, rows)
    masks = jnp.concatenate(
        [((own >= o * owned) & (own < (o + 1) * owned)).astype(F32) for o in range(owners)], axis=0
    )
    ranks = jnp.dot(masks.astype(BF16), upto, preferred_element_type=F32) - 1.0
    slots = jnp.zeros((users, rows), F32)
    for o in range(owners):
        part = slice(o * users, (o + 1) * users)
        slots = slots + masks[part] * (ranks[part] + float(o * cap))
    slot_ref[...] = slots.astype(jnp.int32).reshape(users, 1, rows)
    ids_all[my_dp] = ids_ref[...]
    for copy in copies:
        copy.wait()
    wanted = ids_all[...].reshape(owners * users, rows) - my_dp * owned
    mine = ((wanted >= 0) & (wanted < owned)).astype(F32)
    rank = jnp.dot(mine.astype(BF16), upto, preferred_element_type=F32)
    rank = jnp.where(mine > 0.0, rank - 1.0, -1.0).astype(jnp.int32)
    digits = [wanted & 255, (wanted >> 8) & 255, (wanted >> 16) & 255]
    slot_iota = lax.broadcasted_iota(jnp.int32, (cap, rows), 0)
    lines = []
    for n in range(owners * users):
        hot = (rank[n : n + 1] == slot_iota).astype(BF16)
        digit = jnp.concatenate([d[n : n + 1] for d in digits] + [jnp.zeros((5, rows), jnp.int32)], axis=0)
        found = lax.dot_general(
            digit.astype(F32).astype(BF16), hot, (((1,), (1,)), ((), ())), preferred_element_type=F32
        )
        lines.append(found[0:1] + 256.0 * found[1:2] + 65536.0 * found[2:3])
    index_ref[...] = jnp.concatenate(lines, axis=0).astype(jnp.int32)


def layer_kernel(
    owners, group, lengths_ref, picked_ref, slot_ref, w_in_ref, w_out_ref, out_ref,
    rows_all, w_in_t, embedded_all, gate_all, send_all, recv_all, ret_all, attn_all,
    q_nat, v_nat, k_lane,
    z_send, z_recv, c_send, c_recv, r_send, r_recv,
):
    _, users, cap, width = picked_ref.shape
    rows = slot_ref.shape[2]
    size = width // HEADS
    per_round = group // HEADS
    rounds = users // per_round
    my_dp, my_ctx = lax.axis_index("dp"), lax.axis_index("ctx")
    my_user, my_head = my_ctx // HEADS, lax.rem(my_ctx, HEADS)
    greet("dp", owners, my_dp, my_ctx)
    greet("ctx", group, my_ctx, my_dp)
    pl.semaphore_wait(pltpu.get_barrier_semaphore(), owners + group - 2)

    def row_copy(u, step):
        peer = lax.rem(my_dp + step, owners)
        return pltpu.make_async_remote_copy(
            src_ref=picked_ref.at[peer, u],
            dst_ref=rows_all.at[u, my_dp],
            send_sem=z_send.at[u, step],
            recv_sem=z_recv.at[u, step],
            device_id=(peer, my_ctx),
            device_id_type=MESH,
        )

    def unit_copy(r, step):
        peer = lax.rem(my_ctx + step, group)
        return pltpu.make_async_remote_copy(
            src_ref=send_all.at[r * per_round + peer // HEADS, lax.rem(peer, HEADS)],
            dst_ref=recv_all.at[r, my_ctx],
            send_sem=c_send.at[r, step],
            recv_sem=c_recv.at[r, step],
            device_id=(my_dp, peer),
            device_id_type=MESH,
        )

    def back_copy(r, step):
        peer = lax.rem(my_ctx + step, group)
        return pltpu.make_async_remote_copy(
            src_ref=ret_all.at[r, peer],
            dst_ref=attn_all.at[r * per_round + my_user, my_head],
            send_sem=r_send.at[r, step],
            recv_sem=r_recv.at[r, step],
            device_id=(my_dp, peer),
            device_id_type=MESH,
        )

    for u in range(users):
        for step in range(1, owners):
            row_copy(u, step).start()
    for u in range(users):
        rows_all[u, my_dp] = picked_ref[my_dp, u]
    for part in range(4):
        cols = slice(part * width, (part + 1) * width)
        w_in_t[cols, :] = w_in_ref[:, cols].T

    def project(u):
        for step in range(1, owners):
            row_copy(u, step).wait_recv()
        found = rows_all[u].reshape(owners * cap, width)
        slot_iota = lax.broadcasted_iota(jnp.int32, (owners * cap, rows), 0)
        hot = (slot_ref[u] == slot_iota).astype(BF16)
        embedded = lax.dot_general(hot, found, (((0,), (0,)), ((), ())), preferred_element_type=F32)
        embedded_all[u] = embedded.astype(BF16)
        center = embedded - jnp.mean(embedded, axis=-1, keepdims=True)
        spread = jnp.mean(center * center, axis=-1, keepdims=True)
        normed = (center * lax.rsqrt(spread + 1e-05)).astype(BF16)

        def part_of(part):
            half = 0.5 * lax.dot_general(
                w_in_t[part * width : (part + 1) * width, :],
                normed,
                (((1,), (1,)), ((), ())),
                preferred_element_type=F32,
            )
            return half_silu(half).astype(BF16)

        scale = 0.5 / math.sqrt(size)
        query = (part_of(2).astype(F32) * scale).astype(BF16)
        send_all[u, :, 0:size, :] = query.reshape(HEADS, size, rows)
        send_all[u, :, size : 2 * size, :] = part_of(3).reshape(HEADS, size, rows)
        send_all[u, :, 2 * size : 3 * size, :] = part_of(1).reshape(HEADS, size, rows)
        gate_all[u] = part_of(0)

    def attend(r):
        length = lengths_ref[r * per_round + my_user]
        for j in range(group):
            block = slice(j * rows, (j + 1) * rows)
            q_nat[block, :] = recv_all[r, j, 0:size, :].T
            k_lane[:, block] = recv_all[r, j, size : 2 * size, :]
            position = j * rows + lax.broadcasted_iota(jnp.int32, (size, rows), 1)
            value = recv_all[r, j, 2 * size : 3 * size, :].astype(F32)
            v_nat[block, :] = jnp.where(position < length, value, 0.0).T.astype(BF16)
        query_pos = lax.broadcasted_iota(jnp.int32, (rows, rows), 0)
        key_pos = lax.broadcasted_iota(jnp.int32, (rows, rows), 1)
        for i in range(group):
            query = q_nat[i * rows : (i + 1) * rows, :]
            total = jnp.zeros((rows, size), F32)
            for j in range(i + 1):
                block = slice(j * rows, (j + 1) * rows)
                half = jnp.dot(query, k_lane[:, block], preferred_element_type=F32)
                weight = half_silu(half)
                if j == i:
                    weight = jnp.where(key_pos <= query_pos, weight, 0.0)
                total = total + jnp.dot(weight.astype(BF16), v_nat[block, :], preferred_element_type=F32)
            ret_all[r, i] = total.T.astype(BF16)

    def finish(u):
        attended = attn_all[u].reshape(width, rows).astype(F32)
        center = attended - jnp.mean(attended, axis=0, keepdims=True)
        spread = jnp.mean(center * center, axis=0, keepdims=True)
        gated = (center * lax.rsqrt(spread + 1e-05) * gate_all[u].astype(F32)).astype(BF16)
        mixed = lax.dot_general(gated, w_out_ref[...], (((0,), (0,)), ((), ())), preferred_element_type=F32)
        out_ref[u] = (embedded_all[u].astype(F32) + mixed).astype(BF16)

    def step_body(t, carry):
        @pl.when(t < rounds)
        def _():
            for k in range(per_round):
                project(t * per_round + k)
            for step in range(1, group):
                unit_copy(t, step).start()
            recv_all[t, my_ctx] = send_all[t * per_round + my_user, my_head]

        @pl.when((t >= 1) & (t <= rounds))
        def _():
            r = t - 1
            for step in range(1, group):
                unit_copy(r, step).wait_recv()
            attend(r)
            for step in range(1, group):
                back_copy(r, step).start()
            attn_all[r * per_round + my_user, my_head] = ret_all[r, my_ctx]

        @pl.when(t >= 2)
        def _():
            r = t - 2
            for step in range(1, group):
                back_copy(r, step).wait_recv()
            for k in range(per_round):
                finish(r * per_round + k)

        return carry

    lax.fori_loop(0, rounds + 2, step_body, 0)
    for u in range(users):
        for step in range(1, owners):
            row_copy(u, step).wait_send()
    for r in range(rounds):
        for step in range(1, group):
            unit_copy(r, step).wait_send()
            back_copy(r, step).wait_send()


def per_device(item_ids, lengths, table, w_in, w_out):
    users, rows = item_ids.shape
    owned, width = table.shape
    owners, group = lax.axis_size("dp"), lax.axis_size("ctx")
    cap = 2 * rows // owners
    size = width // HEADS
    per_round = group // HEADS
    rounds = users // per_round
    vmem = pl.BlockSpec(memory_space=pltpu.VMEM)
    index, slots = pl.pallas_call(
        functools.partial(index_kernel, owners, owned, cap),
        out_shape=(
            jax.ShapeDtypeStruct((owners * users, cap), jnp.int32),
            jax.ShapeDtypeStruct((users, 1, rows), jnp.int32),
        ),
        in_specs=[vmem],
        out_specs=(vmem, vmem),
        scratch_shapes=[
            pltpu.VMEM((owners, users, 1, rows), jnp.int32),
            pltpu.SemaphoreType.DMA((owners,)),
            pltpu.SemaphoreType.DMA((owners,)),
        ],
        compiler_params=pltpu.CompilerParams(collective_id=0, has_side_effects=True),
    )(item_ids.reshape(users, 1, rows))
    picked = jnp.take(table, index.reshape(-1), axis=0, mode="clip").reshape(owners, users, cap, width)
    return pl.pallas_call(
        functools.partial(layer_kernel, owners, group),
        out_shape=jax.ShapeDtypeStruct((users, rows, width), BF16),
        in_specs=[pl.BlockSpec(memory_space=pltpu.SMEM), vmem, vmem, vmem, vmem],
        out_specs=vmem,
        scratch_shapes=[
            pltpu.VMEM((users, owners, cap, width), BF16),
            pltpu.VMEM((4 * width, width), BF16),
            pltpu.VMEM((users, rows, width), BF16),
            pltpu.VMEM((users, width, rows), BF16),
            pltpu.VMEM((users, HEADS, 3 * size, rows), BF16),
            pltpu.VMEM((rounds, group, 3 * size, rows), BF16),
            pltpu.VMEM((rounds, group, size, rows), BF16),
            pltpu.VMEM((users, HEADS, size, rows), BF16),
            pltpu.VMEM((group * rows, size), BF16),
            pltpu.VMEM((group * rows, size), BF16),
            pltpu.VMEM((size, group * rows), BF16),
            pltpu.SemaphoreType.DMA((users, owners)),
            pltpu.SemaphoreType.DMA((users, owners)),
            pltpu.SemaphoreType.DMA((rounds, group)),
            pltpu.SemaphoreType.DMA((rounds, group)),
            pltpu.SemaphoreType.DMA((rounds, group)),
            pltpu.SemaphoreType.DMA((rounds, group)),
        ],
        compiler_params=pltpu.CompilerParams(
            collective_id=1, has_side_effects=True, vmem_limit_bytes=56 * 1024 * 1024
        ),
    )(lengths, picked, slots, w_in, w_out)


def solution(mesh):
    return jax.shard_map(
        per_device,
        mesh=mesh,
        in_specs=(P("dp", "ctx"), P("dp"), P("dp", None), P(), P()),
        out_specs=P("dp", "ctx", None),
        check_vma=False,
    )
```

```python
import functools
import math

import jax
import jax.numpy as jnp
from jax import lax
from jax.experimental import pallas as pl
from jax.experimental.pallas import tpu as pltpu
from jax.sharding import PartitionSpec as P

HEADS = 8
F32 = jnp.float32
BF16 = jnp.bfloat16
MESH = pl.DeviceIdType.MESH


def half_silu(h):
    return h + h * jnp.tanh(h)


def greet(axis, size, me, other):
    barrier = pltpu.get_barrier_semaphore()
    for step in range(1, size):
        peer = lax.rem(me + step, size)
        device = (peer, other) if axis == "dp" else (other, peer)
        pl.semaphore_signal(barrier, inc=1, device_id=device, device_id_type=MESH)


def layer_kernel(
    owners, group, lengths_ref, ids_ref, table_ref, w_in_ref, w_out_ref, out_ref,
    ids_all, slot_all, index_vmem, index_smem, table_chunk, table_wide, row_wide, picked,
    w_in_all, w_out_all, rows_all, w_in_t, embedded_all, gate_all, send_all, recv_all,
    ret_all, attn_all, q_nat, v_nat, k_lane,
    t_sem, w_sem, i_sem, n_send, n_recv, z_send, z_recv, c_send, c_recv, r_send, r_recv,
):
    owned, width = table_ref.shape
    users, rows = ids_ref.shape
    cap = row_wide.shape[0]
    size = width // HEADS
    per_round = group // HEADS
    rounds = users // per_round
    depth, chunk = table_chunk.shape[:2]
    chunks = owned // chunk
    my_dp, my_ctx = lax.axis_index("dp"), lax.axis_index("ctx")
    my_user, my_head = my_ctx // HEADS, lax.rem(my_ctx, HEADS)

    def table_copy(c):
        return pltpu.make_async_copy(
            table_ref.at[pl.ds(pl.multiple_of(c * chunk, chunk), chunk), :],
            table_chunk.at[lax.rem(c, depth)],
            t_sem.at[lax.rem(c, depth)],
        )

    for c in range(depth):
        table_copy(c).start()
    greet("dp", owners, my_dp, my_ctx)
    greet("ctx", group, my_ctx, my_dp)
    pl.semaphore_wait(pltpu.get_barrier_semaphore(), owners + group - 2)

    def id_copy(step):
        return pltpu.make_async_remote_copy(
            src_ref=ids_ref,
            dst_ref=ids_all.at[my_dp],
            send_sem=n_send.at[step],
            recv_sem=n_recv.at[step],
            device_id=(lax.rem(my_dp + step, owners), my_ctx),
            device_id_type=MESH,
        )

    for step in range(1, owners):
        id_copy(step).start()

    def widen(c, carry):
        table_copy(c).wait()
        table_wide[pl.ds(pl.multiple_of(c * chunk, chunk), chunk), :] = table_chunk[lax.rem(c, depth)].astype(F32)

        @pl.when(c + depth < chunks)
        def _():
            table_copy(c + depth).start()

        return carry

    lax.fori_loop(0, chunks, widen, 0)
    w_in_copy = pltpu.make_async_copy(w_in_ref, w_in_all, w_sem.at[0])
    w_out_copy = pltpu.make_async_copy(w_out_ref, w_out_all, w_sem.at[1])
    w_in_copy.start()
    w_out_copy.start()

    earlier = lax.broadcasted_iota(jnp.int32, (rows, rows), 0)
    later = lax.broadcasted_iota(jnp.int32, (rows, rows), 1)
    upto = (earlier <= later).astype(BF16)
    own = ids_ref[...]
    ids_all[my_dp] = own
    for step in range(1, owners):
        id_copy(step).wait_recv()
    wanted = jnp.concatenate([ids_all[o] for o in range(owners)], axis=0) - my_dp * owned
    mine = ((wanted >= 0) & (wanted < owned)).astype(F32)
    rank = jnp.dot(mine.astype(BF16), upto, preferred_element_type=F32)
    rank = jnp.where(mine > 0.0, rank - 1.0, -1.0).astype(jnp.int32)
    digits = [wanted & 255, (wanted >> 8) & 255, (wanted >> 16) & 255]
    slot_iota = lax.broadcasted_iota(jnp.int32, (cap, rows), 0)
    lines = []
    for n in range(owners * users):
        hot = (rank[n : n + 1] == slot_iota).astype(BF16)
        digit = jnp.concatenate([d[n : n + 1] for d in digits] + [jnp.zeros((5, rows), jnp.int32)], axis=0)
        found = lax.dot_general(
            digit.astype(F32).astype(BF16), hot, (((1,), (1,)), ((), ())), preferred_element_type=F32
        )
        lines.append(found[0:1] + 256.0 * found[1:2] + 65536.0 * found[2:3])
    index_vmem[...] = jnp.concatenate(lines, axis=0).astype(jnp.int32)
    index_copy = pltpu.make_async_copy(index_vmem, index_smem, i_sem)
    index_copy.start()
    masks = jnp.concatenate(
        [((own >= o * owned) & (own < (o + 1) * owned)).astype(F32) for o in range(owners)], axis=0
    )
    ranks = jnp.dot(masks.astype(BF16), upto, preferred_element_type=F32) - 1.0
    slots = jnp.zeros((users, rows), F32)
    for o in range(owners):
        part = slice(o * users, (o + 1) * users)
        slots = slots + masks[part] * (ranks[part] + float(o * cap))
    slots = slots.astype(jnp.int32)
    for u in range(users):
        slot_all[u] = slots[u : u + 1]
    index_copy.wait()

    def row_copy(u, step):
        peer = lax.rem(my_dp + step, owners)
        return pltpu.make_async_remote_copy(
            src_ref=picked.at[u, step],
            dst_ref=rows_all.at[u, my_dp],
            send_sem=z_send.at[u, step],
            recv_sem=z_recv.at[u, step],
            device_id=(peer, my_ctx),
            device_id_type=MESH,
        )

    def pick(u, step):
        line = lax.rem(my_dp + step, owners) * users + u
        batch = 16

        def pick_batch(k, carry):
            base = pl.multiple_of(k * batch, batch)
            for n in range(batch):
                row = jnp.clip(index_smem[line, base + n], 0, owned - 1)
                row_wide[pl.ds(base + n, 1), :] = table_wide[pl.ds(row, 1), :]
            return carry

        lax.fori_loop(0, cap // batch, pick_batch, 0)
        return row_wide[...].astype(BF16)

    def pick_user(u, carry):
        for step in range(1, owners):
            picked[u, step] = pick(u, step)
            row_copy(u, step).start()
        rows_all[u, my_dp] = pick(u, 0)
        return carry

    lax.fori_loop(0, users, pick_user, 0)
    w_in_copy.wait()
    w_out_copy.wait()
    for part in range(4):
        cols = slice(part * width, (part + 1) * width)
        w_in_t[cols, :] = w_in_all[:, cols].T

    def unit_copy(r, step):
        peer = lax.rem(my_ctx + step, group)
        return pltpu.make_async_remote_copy(
            src_ref=send_all.at[r * per_round + peer // HEADS, lax.rem(peer, HEADS)],
            dst_ref=recv_all.at[r, my_ctx],
            send_sem=c_send.at[r, step],
            recv_sem=c_recv.at[r, step],
            device_id=(my_dp, peer),
            device_id_type=MESH,
        )

    def back_copy(r, peer, sender):
        return pltpu.make_async_remote_copy(
            src_ref=ret_all.at[r, peer],
            dst_ref=attn_all.at[r * per_round + my_user, my_head],
            send_sem=r_send.at[r, peer],
            recv_sem=r_recv.at[r, sender],
            device_id=(my_dp, peer),
            device_id_type=MESH,
        )

    def part_of(part, normed):
        half = 0.5 * lax.dot_general(
            w_in_t[part * width : (part + 1) * width, :],
            normed,
            (((1,), (1,)), ((), ())),
            preferred_element_type=F32,
        )
        return half_silu(half).astype(BF16)

    def project(u):
        for step in range(1, owners):
            row_copy(u, step).wait_recv()
        found = rows_all[u].reshape(owners * cap, width)
        slot_iota = lax.broadcasted_iota(jnp.int32, (owners * cap, rows), 0)
        hot = (slot_all[u] == slot_iota).astype(BF16)
        embedded = lax.dot_general(hot, found, (((0,), (0,)), ((), ())), preferred_element_type=F32)
        embedded_all[u] = embedded.astype(BF16)
        center = embedded - jnp.mean(embedded, axis=-1, keepdims=True)
        spread = jnp.mean(center * center, axis=-1, keepdims=True)
        normed = (center * lax.rsqrt(spread + 1e-05)).astype(BF16)

        scale = 0.5 / math.sqrt(size)
        query = (part_of(2, normed).astype(F32) * scale).astype(BF16)
        send_all[u, :, 0:size, :] = query.reshape(HEADS, size, rows)
        send_all[u, :, size : 2 * size, :] = part_of(3, normed).reshape(HEADS, size, rows)
        send_all[u, :, 2 * size : 3 * size, :] = part_of(1, normed).reshape(HEADS, size, rows)
        return normed

    def attend(r):
        length = lengths_ref[r * per_round + my_user]
        for j in range(group):
            block = slice(j * rows, (j + 1) * rows)
            q_nat[block, :] = recv_all[r, j, 0:size, :].T
            k_lane[:, block] = recv_all[r, j, size : 2 * size, :]
            position = j * rows + lax.broadcasted_iota(jnp.int32, (size, rows), 1)
            value = recv_all[r, j, 2 * size : 3 * size, :].astype(F32)
            v_nat[block, :] = jnp.where(position < length, value, 0.0).T.astype(BF16)
        query_pos = lax.broadcasted_iota(jnp.int32, (rows, rows), 0)
        key_pos = lax.broadcasted_iota(jnp.int32, (rows, rows), 1)
        extra_row = lax.broadcasted_iota(jnp.int32, (ret_all.shape[2] - size, rows), 0)
        for i in range(group):
            query = q_nat[i * rows : (i + 1) * rows, :]
            total = jnp.zeros((rows, size), F32)
            for j in range(i + 1):
                block = slice(j * rows, (j + 1) * rows)
                half = jnp.dot(query, k_lane[:, block], preferred_element_type=F32)
                weight = half_silu(half)
                if j == i:
                    weight = jnp.where(key_pos <= query_pos, weight, 0.0)
                total = total + jnp.dot(weight.astype(BF16), v_nat[block, :], preferred_element_type=F32)
            total = total.T
            middle = jnp.mean(total, axis=0, keepdims=True)
            high = middle.astype(BF16).astype(F32)
            low = (middle - high).astype(BF16).astype(F32)
            extra = jnp.where(extra_row == 0, high, jnp.where(extra_row == 1, low, 0.0))
            extra = jnp.where(extra_row == 2, middle - high - low, extra)
            ret_all[r, i, 0:size, :] = (total - middle).astype(BF16)
            ret_all[r, i, size:, :] = extra.astype(BF16)

            @pl.when(my_ctx != i)
            def _():
                back_copy(r, i, my_ctx).start()


    def finish(u):
        middle = jnp.sum(attn_all[u, :, size:, :].astype(F32), axis=1, keepdims=True)
        middle = middle - jnp.mean(middle, axis=0, keepdims=True)
        attended = (attn_all[u, :, 0:size, :].astype(F32) + middle).reshape(width, rows)
        center = attended - jnp.mean(attended, axis=0, keepdims=True)
        spread = jnp.mean(center * center, axis=0, keepdims=True)
        gated = (center * lax.rsqrt(spread + 1e-05) * gate_all[u].astype(F32)).astype(BF16)
        mixed = lax.dot_general(gated, w_out_all[...], (((0,), (0,)), ((), ())), preferred_element_type=F32)
        out_ref[u] = (embedded_all[u].astype(F32) + mixed).astype(BF16)

    def step_body(t, carry):
        @pl.when(t < rounds)
        def _():
            normed = [project(t * per_round + k) for k in range(per_round)]
            for step in range(1, group):
                unit_copy(t, step).start()
            for k in range(per_round):
                gate_all[t * per_round + k] = part_of(0, normed[k])
            recv_all[t, my_ctx] = send_all[t * per_round + my_user, my_head]

        @pl.when((t >= 1) & (t <= rounds))
        def _():
            r = t - 1
            for step in range(1, group):
                unit_copy(r, step).wait_recv()
            attend(r)
            attn_all[r * per_round + my_user, my_head] = ret_all[r, my_ctx]

        @pl.when(t >= 2)
        def _():
            r = t - 2
            for step in range(1, group):
                sender = lax.rem(my_ctx + step, group)
                back_copy(r, sender, sender).wait_recv()
            for k in range(per_round):
                finish(r * per_round + k)

        return carry

    lax.fori_loop(0, rounds + 2, step_body, 0)
    for step in range(1, owners):
        id_copy(step).wait_send()
    for u in range(users):
        for step in range(1, owners):
            row_copy(u, step).wait_send()
    for r in range(rounds):
        for step in range(1, group):
            unit_copy(r, step).wait_send()
            back_copy(r, lax.rem(my_ctx + step, group), my_ctx).wait_send()


def per_device(item_ids, lengths, table, w_in, w_out):
    users, rows = item_ids.shape
    owned, width = table.shape
    owners, group = lax.axis_size("dp"), lax.axis_size("ctx")
    cap = 2 * rows // owners
    size = width // HEADS
    per_round = group // HEADS
    rounds = users // per_round
    total = group * rows
    chunk = math.gcd(owned, 512)
    depth = min(4, owned // chunk)
    back = size + 16
    vmem = pl.BlockSpec(memory_space=pltpu.VMEM)
    hbm = pl.BlockSpec(memory_space=pl.ANY)
    dma = pltpu.SemaphoreType.DMA
    return pl.pallas_call(
        functools.partial(layer_kernel, owners, group),
        out_shape=jax.ShapeDtypeStruct((users, rows, width), BF16),
        in_specs=[pl.BlockSpec(memory_space=pltpu.SMEM), vmem, hbm, hbm, hbm],
        out_specs=vmem,
        scratch_shapes=[
            pltpu.VMEM((owners, users, rows), jnp.int32),
            pltpu.VMEM((users, 1, rows), jnp.int32),
            pltpu.VMEM((owners * users, cap), jnp.int32),
            pltpu.SMEM((owners * users, cap), jnp.int32),
            pltpu.VMEM((depth, chunk, width), BF16),
            pltpu.VMEM((owned, width), F32),
            pltpu.VMEM((cap, width), F32),
            pltpu.VMEM((users, owners, cap, width), BF16),
            pltpu.VMEM((width, 4 * width), BF16),
            pltpu.VMEM((width, width), BF16),
            pltpu.VMEM((users, owners, cap, width), BF16),
            pltpu.VMEM((4 * width, width), BF16),
            pltpu.VMEM((users, rows, width), BF16),
            pltpu.VMEM((users, width, rows), BF16),
            pltpu.VMEM((users, HEADS, 3 * size, rows), BF16),
            pltpu.VMEM((rounds, group, 3 * size, rows), BF16),
            pltpu.VMEM((rounds, group, back, rows), BF16),
            pltpu.VMEM((users, HEADS, back, rows), BF16),
            pltpu.VMEM((total, size), BF16),
            pltpu.VMEM((total, size), BF16),
            pltpu.VMEM((size, total), BF16),
            dma((depth,)),
            dma((2,)),
            dma,
            dma((owners,)),
            dma((owners,)),
            dma((users, owners)),
            dma((users, owners)),
            dma((rounds, group)),
            dma((rounds, group)),
            dma((rounds, group)),
            dma((rounds, group)),
        ],
        compiler_params=pltpu.CompilerParams(
            collective_id=0, has_side_effects=True, vmem_limit_bytes=67_043_328
        ),
    )(lengths, item_ids, table, w_in, w_out)


def solution(mesh):
    return jax.shard_map(
        per_device,
        mesh=mesh,
        in_specs=(P("dp", "ctx"), P("dp"), P("dp", None), P(), P()),
        out_specs=P("dp", "ctx", None),
        check_vma=False,
    )
```

```python
import functools
import math

import jax
import jax.numpy as jnp
from jax import lax
from jax.experimental import pallas as pl
from jax.experimental.pallas import tpu as pltpu
from jax.sharding import PartitionSpec as P

HEADS = 8
F32 = jnp.float32
BF16 = jnp.bfloat16
MESH = pl.DeviceIdType.MESH


def half_silu(h):
    return h + h * jnp.tanh(h)


def greet(axis, size, me, other):
    barrier = pltpu.get_barrier_semaphore()
    for step in range(1, size):
        peer = lax.rem(me + step, size)
        device = (peer, other) if axis == "dp" else (other, peer)
        pl.semaphore_signal(barrier, inc=1, device_id=device, device_id_type=MESH)


def layer_kernel(
    owners, group, lengths_ref, ids_ref, table_ref, w_in_ref, w_out_ref, out_ref,
    ids_all, slot_all, index_vmem, index_smem, table_chunk, table_wide, row_wide, picked,
    w_in_all, w_out_all, rows_all, w_in_t, embedded_all, gate_all, send_all, recv_all,
    ret_all, attn_all, q_nat, v_nat, k_lane,
    t_sem, w_sem, i_sem, n_send, n_recv, z_send, z_recv, c_send, c_recv, r_send, r_recv,
):
    owned, width = table_ref.shape
    users, rows = ids_ref.shape
    cap = row_wide.shape[0]
    size = width // HEADS
    per_round = group // HEADS
    rounds = users // per_round
    depth, chunk = table_chunk.shape[:2]
    chunks = owned // chunk
    my_dp, my_ctx = lax.axis_index("dp"), lax.axis_index("ctx")
    my_user, my_head = my_ctx // HEADS, lax.rem(my_ctx, HEADS)

    def table_copy(c):
        return pltpu.make_async_copy(
            table_ref.at[pl.ds(pl.multiple_of(c * chunk, chunk), chunk), :],
            table_chunk.at[lax.rem(c, depth)],
            t_sem.at[lax.rem(c, depth)],
        )

    for c in range(depth):
        table_copy(c).start()
    greet("dp", owners, my_dp, my_ctx)
    greet("ctx", group, my_ctx, my_dp)
    pl.semaphore_wait(pltpu.get_barrier_semaphore(), owners + group - 2)

    def id_copy(step):
        return pltpu.make_async_remote_copy(
            src_ref=ids_ref,
            dst_ref=ids_all.at[my_dp],
            send_sem=n_send.at[step],
            recv_sem=n_recv.at[step],
            device_id=(lax.rem(my_dp + step, owners), my_ctx),
            device_id_type=MESH,
        )

    for step in range(1, owners):
        id_copy(step).start()

    def widen(c, carry):
        table_copy(c).wait()
        table_wide[pl.ds(pl.multiple_of(c * chunk, chunk), chunk), :] = table_chunk[lax.rem(c, depth)].astype(F32)

        @pl.when(c + depth < chunks)
        def _():
            table_copy(c + depth).start()

        return carry

    lax.fori_loop(0, chunks, widen, 0)
    w_in_copy = pltpu.make_async_copy(w_in_ref, w_in_all, w_sem.at[0])
    w_out_copy = pltpu.make_async_copy(w_out_ref, w_out_all, w_sem.at[1])
    w_in_copy.start()
    w_out_copy.start()

    earlier = lax.broadcasted_iota(jnp.int32, (rows, rows), 0)
    later = lax.broadcasted_iota(jnp.int32, (rows, rows), 1)
    upto = (earlier <= later).astype(BF16)
    own = ids_ref[...]
    ids_all[my_dp] = own
    for step in range(1, owners):
        id_copy(step).wait_recv()
    wanted = jnp.concatenate([ids_all[o] for o in range(owners)], axis=0) - my_dp * owned
    mine = ((wanted >= 0) & (wanted < owned)).astype(F32)
    rank = jnp.dot(mine.astype(BF16), upto, preferred_element_type=F32)
    rank = jnp.where(mine > 0.0, rank - 1.0, -1.0).astype(jnp.int32)
    digits = [wanted & 255, (wanted >> 8) & 255, (wanted >> 16) & 255]
    slot_iota = lax.broadcasted_iota(jnp.int32, (cap, rows), 0)
    lines = []
    for n in range(owners * users):
        hot = (rank[n : n + 1] == slot_iota).astype(BF16)
        digit = jnp.concatenate([d[n : n + 1] for d in digits] + [jnp.zeros((5, rows), jnp.int32)], axis=0)
        found = lax.dot_general(
            digit.astype(F32).astype(BF16), hot, (((1,), (1,)), ((), ())), preferred_element_type=F32
        )
        lines.append(found[0:1] + 256.0 * found[1:2] + 65536.0 * found[2:3])
    index_vmem[...] = jnp.concatenate(lines, axis=0).astype(jnp.int32)
    index_copy = pltpu.make_async_copy(index_vmem, index_smem, i_sem)
    index_copy.start()
    masks = jnp.concatenate(
        [((own >= o * owned) & (own < (o + 1) * owned)).astype(F32) for o in range(owners)], axis=0
    )
    ranks = jnp.dot(masks.astype(BF16), upto, preferred_element_type=F32) - 1.0
    slots = jnp.zeros((users, rows), F32)
    for o in range(owners):
        part = slice(o * users, (o + 1) * users)
        slots = slots + masks[part] * (ranks[part] + float(o * cap))
    slots = slots.astype(jnp.int32)
    for u in range(users):
        slot_all[u] = slots[u : u + 1]
    index_copy.wait()

    def row_copy(u, step):
        peer = lax.rem(my_dp + step, owners)
        return pltpu.make_async_remote_copy(
            src_ref=picked.at[u, step],
            dst_ref=rows_all.at[u, my_dp],
            send_sem=z_send.at[u, step],
            recv_sem=z_recv.at[u, step],
            device_id=(peer, my_ctx),
            device_id_type=MESH,
        )

    def pick(u, step):
        line = lax.rem(my_dp + step, owners) * users + u
        batch = 16

        def pick_batch(k, carry):
            base = pl.multiple_of(k * batch, batch)
            for n in range(batch):
                row = jnp.clip(index_smem[line, base + n], 0, owned - 1)
                row_wide[pl.ds(base + n, 1), :] = table_wide[pl.ds(row, 1), :]
            return carry

        lax.fori_loop(0, cap // batch, pick_batch, 0)
        return row_wide[...].astype(BF16)

    def pick_user(u, carry):
        for step in range(1, owners):
            picked[u, step] = pick(u, step)
            row_copy(u, step).start()
        rows_all[u, my_dp] = pick(u, 0)
        return carry

    lax.fori_loop(0, users, pick_user, 0)
    w_in_copy.wait()
    w_out_copy.wait()
    for part in range(4):
        cols = slice(part * width, (part + 1) * width)
        w_in_t[cols, :] = w_in_all[:, cols].T

    def unit_copy(r, step):
        peer = lax.rem(my_ctx + step, group)
        return pltpu.make_async_remote_copy(
            src_ref=send_all.at[r * per_round + peer // HEADS, lax.rem(peer, HEADS)],
            dst_ref=recv_all.at[r, my_ctx],
            send_sem=c_send.at[r, step],
            recv_sem=c_recv.at[r, step],
            device_id=(my_dp, peer),
            device_id_type=MESH,
        )

    def back_copy(r, peer, sender):
        return pltpu.make_async_remote_copy(
            src_ref=ret_all.at[r, peer],
            dst_ref=attn_all.at[r * per_round + my_user, my_head],
            send_sem=r_send.at[r, peer],
            recv_sem=r_recv.at[r, sender],
            device_id=(my_dp, peer),
            device_id_type=MESH,
        )

    def part_of(part, normed):
        half = 0.5 * lax.dot_general(
            w_in_t[part * width : (part + 1) * width, :],
            normed,
            (((1,), (1,)), ((), ())),
            preferred_element_type=F32,
        )
        return half_silu(half).astype(BF16)

    def project(u):
        for step in range(1, owners):
            row_copy(u, step).wait_recv()
        found = rows_all[u].reshape(owners * cap, width)
        slot_iota = lax.broadcasted_iota(jnp.int32, (owners * cap, rows), 0)
        hot = (slot_all[u] == slot_iota).astype(BF16)
        embedded = lax.dot_general(hot, found, (((0,), (0,)), ((), ())), preferred_element_type=F32)
        embedded_all[u] = embedded.astype(BF16)
        center = embedded - jnp.mean(embedded, axis=-1, keepdims=True)
        spread = jnp.mean(center * center, axis=-1, keepdims=True)
        normed = (center * lax.rsqrt(spread + 1e-05)).astype(BF16)

        scale = 0.5 / math.sqrt(size)
        query = (part_of(2, normed).astype(F32) * scale).astype(BF16)
        send_all[u, :, 0:size, :] = query.reshape(HEADS, size, rows)
        send_all[u, :, size : 2 * size, :] = part_of(3, normed).reshape(HEADS, size, rows)
        send_all[u, :, 2 * size : 3 * size, :] = part_of(1, normed).reshape(HEADS, size, rows)
        return normed

    def attend(r):
        length = lengths_ref[r * per_round + my_user]
        for j in range(group):
            block = slice(j * rows, (j + 1) * rows)
            q_nat[block, :] = recv_all[r, j, 0:size, :].T
            k_lane[:, block] = recv_all[r, j, size : 2 * size, :]
            position = j * rows + lax.broadcasted_iota(jnp.int32, (size, rows), 1)
            value = recv_all[r, j, 2 * size : 3 * size, :].astype(F32)
            v_nat[block, :] = jnp.where(position < length, value, 0.0).T.astype(BF16)
        query_pos = lax.broadcasted_iota(jnp.int32, (rows, rows), 0)
        key_pos = lax.broadcasted_iota(jnp.int32, (rows, rows), 1)
        extra_row = lax.broadcasted_iota(jnp.int32, (ret_all.shape[2] - size, rows), 0)
        for i in range(group):
            query = q_nat[i * rows : (i + 1) * rows, :]
            total = jnp.zeros((rows, size), F32)
            for j in range(i + 1):
                block = slice(j * rows, (j + 1) * rows)
                half = jnp.dot(query, k_lane[:, block], preferred_element_type=F32)
                weight = half_silu(half)
                if j == i:
                    weight = jnp.where(key_pos <= query_pos, weight, 0.0)
                total = total + jnp.dot(weight.astype(BF16), v_nat[block, :], preferred_element_type=F32)
            total = total.T
            middle = jnp.mean(total, axis=0, keepdims=True)
            high = middle.astype(BF16).astype(F32)
            low = (middle - high).astype(BF16).astype(F32)
            extra = jnp.where(extra_row == 0, high, jnp.where(extra_row == 1, low, 0.0))
            extra = jnp.where(extra_row == 2, middle - high - low, extra)
            ret_all[r, i, 0:size, :] = (total - middle).astype(BF16)
            ret_all[r, i, size:, :] = extra.astype(BF16)

            @pl.when(my_ctx != i)
            def _():
                back_copy(r, i, my_ctx).start()


    def finish(u):
        middle = jnp.sum(attn_all[u, :, size:, :].astype(F32), axis=1, keepdims=True)
        middle = middle - jnp.mean(middle, axis=0, keepdims=True)
        attended = (attn_all[u, :, 0:size, :].astype(F32) + middle).reshape(width, rows)
        center = attended - jnp.mean(attended, axis=0, keepdims=True)
        spread = jnp.mean(center * center, axis=0, keepdims=True)
        gated = (center * lax.rsqrt(spread + 1e-05) * gate_all[u].astype(F32)).astype(BF16)
        mixed = lax.dot_general(gated, w_out_all[...], (((0,), (0,)), ((), ())), preferred_element_type=F32)
        out_ref[u] = (embedded_all[u].astype(F32) + mixed).astype(BF16)

    def step_body(t, carry):
        @pl.when(t < rounds)
        def _():
            normed = [project(t * per_round + k) for k in range(per_round)]
            for step in range(1, group):
                unit_copy(t, step).start()
            for k in range(per_round):
                gate_all[t * per_round + k] = part_of(0, normed[k])
            recv_all[t, my_ctx] = send_all[t * per_round + my_user, my_head]

        @pl.when((t >= 1) & (t <= rounds))
        def _():
            r = t - 1
            for step in range(1, group):
                unit_copy(r, step).wait_recv()
            attend(r)
            attn_all[r * per_round + my_user, my_head] = ret_all[r, my_ctx]

        @pl.when(t >= 2)
        def _():
            r = t - 2
            for step in range(1, group):
                sender = lax.rem(my_ctx + step, group)
                back_copy(r, sender, sender).wait_recv()
            for k in range(per_round):
                finish(r * per_round + k)

        return carry

    lax.fori_loop(0, rounds + 2, step_body, 0)
    for step in range(1, owners):
        id_copy(step).wait_send()
    for u in range(users):
        for step in range(1, owners):
            row_copy(u, step).wait_send()
    for r in range(rounds):
        for step in range(1, group):
            unit_copy(r, step).wait_send()
            back_copy(r, lax.rem(my_ctx + step, group), my_ctx).wait_send()


def per_device(item_ids, lengths, table, w_in, w_out):
    users, rows = item_ids.shape
    owned, width = table.shape
    owners, group = lax.axis_size("dp"), lax.axis_size("ctx")
    cap = 2 * rows // owners
    size = width // HEADS
    per_round = group // HEADS
    rounds = users // per_round
    total = group * rows
    chunk = math.gcd(owned, 512)
    depth = min(8, owned // chunk)
    back = size + 16
    vmem = pl.BlockSpec(memory_space=pltpu.VMEM)
    hbm = pl.BlockSpec(memory_space=pl.ANY)
    dma = pltpu.SemaphoreType.DMA
    return pl.pallas_call(
        functools.partial(layer_kernel, owners, group),
        out_shape=jax.ShapeDtypeStruct((users, rows, width), BF16),
        in_specs=[pl.BlockSpec(memory_space=pltpu.SMEM), vmem, hbm, hbm, hbm],
        out_specs=vmem,
        scratch_shapes=[
            pltpu.VMEM((owners, users, rows), jnp.int32),
            pltpu.VMEM((users, 1, rows), jnp.int32),
            pltpu.VMEM((owners * users, cap), jnp.int32),
            pltpu.SMEM((owners * users, cap), jnp.int32),
            pltpu.VMEM((depth, chunk, width), BF16),
            pltpu.VMEM((owned, width), F32),
            pltpu.VMEM((cap, width), F32),
            pltpu.VMEM((users, owners, cap, width), BF16),
            pltpu.VMEM((width, 4 * width), BF16),
            pltpu.VMEM((width, width), BF16),
            pltpu.VMEM((users, owners, cap, width), BF16),
            pltpu.VMEM((4 * width, width), BF16),
            pltpu.VMEM((users, rows, width), BF16),
            pltpu.VMEM((users, width, rows), BF16),
            pltpu.VMEM((users, HEADS, 3 * size, rows), BF16),
            pltpu.VMEM((rounds, group, 3 * size, rows), BF16),
            pltpu.VMEM((rounds, group, back, rows), BF16),
            pltpu.VMEM((users, HEADS, back, rows), BF16),
            pltpu.VMEM((total, size), BF16),
            pltpu.VMEM((total, size), BF16),
            pltpu.VMEM((size, total), BF16),
            dma((depth,)),
            dma((2,)),
            dma,
            dma((owners,)),
            dma((owners,)),
            dma((users, owners)),
            dma((users, owners)),
            dma((rounds, group)),
            dma((rounds, group)),
            dma((rounds, group)),
            dma((rounds, group)),
        ],
        compiler_params=pltpu.CompilerParams(
            collective_id=0, has_side_effects=True, vmem_limit_bytes=67_043_328
        ),
    )(lengths, item_ids, table, w_in, w_out)


def solution(mesh):
    return jax.shard_map(
        per_device,
        mesh=mesh,
        in_specs=(P("dp", "ctx"), P("dp"), P("dp", None), P(), P()),
        out_specs=P("dp", "ctx", None),
        check_vma=False,
    )
```
